16 devices in a mesh: rep: 1, dp: 16 (over x, y, z, core).
Axes of the slice: x: 2, y: 2, z: 2, core: 2. Of those that a mesh axis runs over, the one named last changes fastest.
Arguments:
- x: bfloat16 [16, 2048, 1024], P(('rep', 'dp'))
- dy: bfloat16 [16, 2048, 1024], P(('rep', 'dp'))
- w_gate: bfloat16 [2, 1024, 6144], replicated
- w_up: bfloat16 [2, 1024, 6144], replicated
- w_down: bfloat16 [2, 6144, 1024], replicated
- m_w_gate: float32 [2, 1024, 6144], P(None, 'dp')
- m_w_up: float32 [2, 1024, 6144], P(None, 'dp')
- m_w_down: float32 [2, 6144, 1024], P(None, 'dp')
- v_w_gate: float32 [2, 1024, 6144], P(None, 'dp')
- v_w_up: float32 [2, 1024, 6144], P(None, 'dp')
- v_w_down: float32 [2, 6144, 1024], P(None, 'dp')
Outputs:
- output 1: bfloat16 [2, 1024, 6144], P('rep')
- output 2: bfloat16 [2, 1024, 6144], P('rep')
- output 3: bfloat16 [2, 6144, 1024], P('rep')
- output 4: float32 [2, 1024, 6144], P('rep', 'dp')
- output 5: float32 [2, 1024, 6144], P('rep', 'dp')
- output 6: float32 [2, 6144, 1024], P('rep', 'dp')
- output 7: float32 [2, 1024, 6144], P('rep', 'dp')
- output 8: float32 [2, 1024, 6144], P('rep', 'dp')
- output 9: float32 [2, 6144, 1024], P('rep', 'dp')
All inputs are finite; a program needn't handle non-finite values.
Results may differ from the reference program's by a relative error of at most 0.022.
Values are sent between devices in bfloat16 or wider.
A program may use at most 2 GiB of HBM per device.

```python
import jax
import jax.numpy as jnp
from jax import lax

SEQUENCES = 16
TOKENS = 2048
D = 1024
FF = 6144
LAYERS = 2
NAMES = ("w_gate", "w_up", "w_down")
SHAPES = {"w_gate": (LAYERS, D, FF), "w_up": (LAYERS, D, FF), "w_down": (LAYERS, FF, D)}


def bump(key, n, height):
    away = (jnp.arange(n, dtype=jnp.int32) - jax.random.randint(key, (), 0, n, jnp.int32)) % n
    return jnp.where(away < n // 8, height, 1.0)


def together(key, own, strength):
    shared = jax.random.normal(key, own.shape[1:], jnp.float32)
    return (own + strength * shared) * lax.rsqrt(1 + strength * strength)


def setup_inputs(seed: int = 0, part: int = 0) -> dict:
    kx, kdy, ka, kb, kz, kf, kh, kl, *keys = jax.random.split(jax.random.key(seed), 8 + 3 * len(NAMES))
    kx, kdy, ka, kb = (jax.random.fold_in(k, part) for k in (kx, kdy, ka, kb))
    kw, km, kv = (keys[i::3] for i in range(3))
    shape = (SEQUENCES, TOKENS, D)
    much_x, much_dy = jax.random.uniform(kz, (2,), jnp.float32, 0.0, 1.0)
    loud = 2.0 ** jax.random.uniform(jax.random.fold_in(kz, 1), (), jnp.float32, -1.0, 2.0)
    layers = 2.0 ** jax.random.uniform(kl, (LAYERS, 1, 1), jnp.float32, -1.0, 1.0)
    x = together(ka, jax.random.normal(kx, shape, jnp.float32), much_x) * bump(kf, D, 4.0)
    dy = together(kb, jax.random.normal(kdy, shape, jnp.float32), much_dy)
    drawn = {"x": x.astype(jnp.bfloat16), "dy": (loud * dy * (SEQUENCES * TOKENS) ** -0.5).astype(jnp.bfloat16)}
    for key, name in zip(kw, NAMES, strict=True):
        w = jax.random.normal(key, SHAPES[name], jnp.float32) * SHAPES[name][1] ** -0.5
        drawn[name] = (w * {"w_gate": 1.0, "w_up": bump(kh, FF, 4.0), "w_down": layers}[name]).astype(jnp.bfloat16)
    for key, name in zip(km, NAMES, strict=True):
        drawn[f"m_{name}"] = 0.1 * jax.random.normal(key, SHAPES[name], jnp.float32)
    for key, name in zip(kv, NAMES, strict=True):
        drawn[f"v_{name}"] = jax.random.uniform(key, SHAPES[name], jnp.float32, 0.005, 0.015)
    return drawn


def matmul(a, w):
    return jnp.dot(a, w, preferred_element_type=jnp.float32).astype(jnp.bfloat16)


def normed(h):
    wide = h.astype(jnp.float32)
    scale = lax.rsqrt(jnp.mean(wide**2, -1, keepdims=True) + 1e-6)
    return (wide * scale).astype(jnp.bfloat16)


def layer(h, w):
    a = normed(h)
    gate = jnp.dot(a, w["w_gate"], preferred_element_type=jnp.float32)
    up = jnp.dot(a, w["w_up"], preferred_element_type=jnp.float32)
    return h + matmul((jax.nn.silu(gate) * up).astype(jnp.bfloat16), w["w_down"])


def adamw(w, m, v, g):
    m = 0.9 * m + 0.1 * g
    v = 0.95 * v + 0.05 * g * g
    step = m * lax.rsqrt(v + 1e-8) + 0.1 * w
    return (w - 0.02 * step).astype(jnp.bfloat16), m, v


def clipped(gradients, sum_of_squares, count):
    factor = jnp.minimum(1.0, 0.5 * lax.rsqrt(sum_of_squares / count + 1e-30))
    return [g * factor for g in gradients]


def stack(weights, h):
    return lax.scan(lambda h, w: (layer(h, w), None), h, weights)[0]


def reference(x, dy, w_gate, w_up, w_down, m_w_gate, m_w_up, m_w_down, v_w_gate, v_w_up, v_w_down):
    weights = dict(zip(NAMES, (w_gate, w_up, w_down), strict=True))

    def take(so_far, sequence):
        h, by_y = sequence
        _, back = jax.vjp(lambda w: stack(w, h), weights)
        return jax.tree.map(lambda total, term: total + term.astype(jnp.float32), so_far, back(by_y)[0]), None

    none_yet = {name: jnp.zeros(w.shape, jnp.float32) for name, w in weights.items()}
    by_weights, _ = lax.scan(take, none_yet, (x, dy))
    gradients = [by_weights[name].astype(jnp.bfloat16).astype(jnp.float32) for name in NAMES]
    gradients = clipped(gradients, sum(jnp.sum(g * g) for g in gradients), sum(g.size for g in gradients))
    new = [
        adamw(w.astype(jnp.float32), m, v, g)
        for w, m, v, g in zip((w_gate, w_up, w_down), (m_w_gate, m_w_up, m_w_down), (v_w_gate, v_w_up, v_w_down), gradients, strict=True)
    ]
    return tuple(one[which] for which in range(3) for one in new)
```

```python
import functools

import jax
import jax.numpy as jnp
from jax import lax
from jax.experimental import pallas as pl
from jax.experimental.pallas import tpu as pltpu
from jax.sharding import PartitionSpec as P

F32, BF16 = jnp.float32, jnp.bfloat16
EPS = 1e-6
MIB = 1 << 20


def dot(a, b, ca, cb):
    return lax.dot_general(a, b, (((ca,), (cb,)), ((), ())), preferred_element_type=F32)


def call(kernel, flops, nbytes, vmem, **kw):
    return pl.pallas_call(
        kernel,
        compiler_params=pltpu.CompilerParams(vmem_limit_bytes=vmem * MIB, dimension_semantics=("arbitrary",)),
        cost_estimate=pl.CostEstimate(flops=flops, bytes_accessed=nbytes, transcendentals=0),
        **kw,
    )


def whole(*shape):
    return pl.BlockSpec(shape, lambda i: (0,) * len(shape), pipeline_mode=pl.Buffered(1))


def normed(h):
    wide = h.astype(F32)
    return (wide * lax.rsqrt(jnp.mean(wide * wide, -1, keepdims=True) + EPS)).astype(BF16)


def gate_up_kernel(a_ref, wg_ref, wu_ref, gate_ref, up_ref, act_ref):
    gate = dot(a_ref[...], wg_ref[0], 1, 0)
    up = dot(a_ref[...], wu_ref[0], 1, 0)
    gate_ref[...] = gate
    up_ref[...] = up
    act_ref[...] = (gate * jax.nn.sigmoid(gate) * up).astype(BF16)


def gate_up(a, wg, wu, bn=256):
    t, d = a.shape
    f = wg.shape[2]
    w = pl.BlockSpec((1, d, bn), lambda j: (0, 0, j))
    o = pl.BlockSpec((t, bn), lambda j: (0, j))
    return call(
        gate_up_kernel, 4 * t * d * f, 10 * t * f + 4 * d * f, 56,
        grid=(f // bn,),
        in_specs=[whole(t, d), w, w],
        out_specs=[o, o, o],
        out_shape=[jax.ShapeDtypeStruct((t, f), F32)] * 2 + [jax.ShapeDtypeStruct((t, f), BF16)],
        name="gate_up",
    )(a, wg, wu)


def down_kernel(act_ref, wd_ref, x_ref, h_ref, a_ref):
    h = x_ref[...] + dot(act_ref[...], wd_ref[0], 1, 0).astype(BF16)
    h_ref[...] = h
    a_ref[...] = normed(h)


def down(act, wd, x, bm=512):
    t, f = act.shape
    d = x.shape[1]
    r = pl.BlockSpec((bm, d), lambda i: (i, 0))
    return call(
        down_kernel, 2 * t * d * f, 2 * (t * f + d * f), 60,
        grid=(t // bm,),
        in_specs=[pl.BlockSpec((bm, f), lambda i: (i, 0)), whole(1, f, d), r],
        out_specs=[r, r],
        out_shape=[jax.ShapeDtypeStruct((t, d), BF16)] * 2,
        name="down",
    )(act, wd, x)


def back_through_product(gate, up, dact):
    dact = dact.astype(BF16).astype(F32)
    sig = jax.nn.sigmoid(gate)
    silu = gate * sig
    dgate = dact * up * (sig + silu * (1.0 - sig))
    return (silu * up).astype(BF16), dgate.astype(BF16), (dact * silu).astype(BF16)


def put_terms(p_ref, stage_g, stage_u, stage_d, sems, j, steps, act, dgate, dup, a, dh, bn):
    n, blocks = p_ref.shape[:2]
    blocks = blocks // 3
    slot = lax.rem(j, 2)
    per = p_ref.shape[3] // bn

    def copies(slot, j):
        out = []
        for which, stage in enumerate((stage_g, stage_u)):
            part = p_ref.at[:, blocks * (1 + which) + lax.div(j, per), :, pl.ds(pl.multiple_of(lax.rem(j, per) * bn, bn), bn)]
            out.append(pltpu.make_async_copy(stage.at[slot], part, sems.at[slot, which]))
        first = j * (bn // 64)
        for i in range(bn // 64):
            to = p_ref.at[lax.div(first + i, blocks), lax.rem(first + i, blocks)]
            out.append(pltpu.make_async_copy(stage_d.at[slot, i], to, sems.at[slot, 2 + i]))
        return out

    @pl.when(j >= 2)
    def _():
        for c in copies(slot, j - 2):
            c.wait()

    for stage, cot in ((stage_g, dgate), (stage_u, dup)):
        stage[slot] = dot(a[...], cot, 0, 0).astype(BF16).reshape(stage.shape[1:])
    stage_d[slot] = dot(act, dh[...], 0, 0).astype(BF16).reshape(stage_d.shape[1:])
    for c in copies(slot, j):
        c.start()

    @pl.when(j == steps - 1)
    def _():
        for c in copies(1 - slot, j - 1) + copies(slot, j):
            c.wait()


def term_scratch(n, d, bn):
    return [
        pltpu.VMEM((2, n, d // n, bn), BF16),
        pltpu.VMEM((2, n, d // n, bn), BF16),
        pltpu.VMEM((2, bn // 64, 64, d), BF16),
        pltpu.SemaphoreType.DMA((2, 2 + bn // 64)),
    ]


def last_layer_kernel(steps, bn, a_ref, dy_ref, wg_ref, wu_ref, wd_ref, dgate_ref, dup_ref, p_ref, *scratch):
    gate = dot(a_ref[...], wg_ref[0], 1, 0)
    up = dot(a_ref[...], wu_ref[0], 1, 0)
    dact = dot(dy_ref[...], wd_ref[0], 1, 1)
    act, dgate, dup = back_through_product(gate, up, dact)
    dgate_ref[...] = dgate
    dup_ref[...] = dup
    put_terms(p_ref, *scratch, pl.program_id(0), steps, act, dgate, dup, a_ref, dy_ref, bn)


def last_layer(a, dy, wg, wu, wd, n, bn=512):
    t, d = a.shape
    f = wg.shape[2]
    last = wg.shape[0] - 1
    steps = f // bn
    w = pl.BlockSpec((1, d, bn), lambda j: (last, 0, j))
    o = pl.BlockSpec((t, bn), lambda j: (0, j))
    return call(
        functools.partial(last_layer_kernel, steps, bn), 12 * t * d * f, 4 * t * f + 12 * d * f, 60,
        grid=(steps,),
        in_specs=[whole(t, d), whole(t, d), w, w, pl.BlockSpec((1, bn, d), lambda j: (last, j, 0))],
        out_specs=[o, o, pl.BlockSpec(memory_space=pl.ANY)],
        out_shape=[jax.ShapeDtypeStruct((t, f), BF16)] * 2 + [jax.ShapeDtypeStruct((n, 3 * f // n // 64, 64, d), BF16)],
        scratch_shapes=term_scratch(n, d, bn),
        name="last_layer",
    )(a, dy, wg, wu, wd)


def to_input_kernel(dgate_ref, dup_ref, wg_ref, wu_ref, h_ref, dy_ref, dh_ref):
    da = dot(dgate_ref[...], wg_ref[0], 1, 1).astype(BF16) + dot(dup_ref[...], wu_ref[0], 1, 1).astype(BF16)
    da = da.astype(F32)
    wide = h_ref[...].astype(F32)
    scale = lax.rsqrt(jnp.mean(wide * wide, -1, keepdims=True) + EPS)
    inner = jnp.mean(da * wide, -1, keepdims=True)
    dwide = da * scale - wide * (scale * scale * scale * inner)
    dh_ref[...] = dy_ref[...] + dwide.astype(BF16)


def to_input(dgate, dup, wg, wu, h, dy, bm=256):
    t, f = dgate.shape
    d = h.shape[1]
    last = wg.shape[0] - 1
    c = pl.BlockSpec((bm, f), lambda i: (i, 0))
    r = pl.BlockSpec((bm, d), lambda i: (i, 0))
    w = pl.BlockSpec((1, d, f), lambda i: (last, 0, 0), pipeline_mode=pl.Buffered(1))
    return call(
        to_input_kernel, 4 * t * d * f, 4 * t * f + 4 * d * f, 60,
        grid=(t // bm,),
        in_specs=[c, c, w, w, r, r],
        out_specs=r,
        out_shape=jax.ShapeDtypeStruct((t, d), BF16),
        name="to_input",
    )(dgate, dup, wg, wu, h, dy)


def first_layer_kernel(steps, bn, gate_ref, up_ref, a_ref, dh_ref, wd_ref, p_ref, *scratch):
    dact = dot(dh_ref[...], wd_ref[0], 1, 1)
    act, dgate, dup = back_through_product(gate_ref[...], up_ref[...], dact)
    put_terms(p_ref, *scratch, pl.program_id(0), steps, act, dgate, dup, a_ref, dh_ref, bn)


def first_layer(gate, up, a, dh, wd, n, bn=512):
    t, d = a.shape
    f = gate.shape[1]
    steps = f // bn
    c = pl.BlockSpec((t, bn), lambda j: (0, j))
    return call(
        functools.partial(first_layer_kernel, steps, bn), 8 * t * d * f, 8 * t * f + 8 * d * f, 60,
        grid=(steps,),
        in_specs=[c, c, whole(t, d), whole(t, d), pl.BlockSpec((1, bn, d), lambda j: (0, j, 0))],
        out_specs=pl.BlockSpec(memory_space=pl.ANY),
        out_shape=jax.ShapeDtypeStruct((n, 3 * f // n // 64, 64, d), BF16),
        scratch_shapes=term_scratch(n, d, bn),
        name="first_layer",
    )(gate, up, a, dh, wd)


ORDERS = ((0, 1, 2), (1, 2, 0), (2, 0, 1))
MESH = pl.DeviceIdType.MESH


def place():
    me = lax.axis_index("dp")
    bits = (lax.rem(me // 8, 2), lax.rem(me // 4, 2), lax.rem(me // 2, 2))
    return me, bits, lax.rem(me, 2)


def neighbour(me, bits, axis):
    step = (8, 4, 2)[axis]
    return {"dp": me + step * (1 - 2 * bits[axis])}


def greet_all(me, n):
    barrier = pltpu.get_barrier_semaphore()

    @pl.loop(1, n)
    def _(i):
        pl.semaphore_signal(barrier, inc=1, device_id={"dp": lax.rem(me + i, n)}, device_id_type=MESH)

    pl.semaphore_wait(barrier, n - 1)


def at(fixed, among):
    return tuple(fixed.get(a, slice(None)) for a in among)


def reduce_kernel(
    n, chunks, p_ref, g1_ref, g_ref, total_ref, own, from_core, from_a, from_b, from_c, square, squares,
    own_sem, core_send, core_recv, a_send, a_recv, b_send, b_recv, c_send, c_recv, sq_send, sq_recv,
):
    me, bits, core = place()
    partner = {"dp": me + 1 - 2 * core}
    slots = own.shape[0]
    greet_all(me, n)

    def own_copy(i, q):
        src = p_ref.at[:, :, :, core, q * chunks + i]
        return pltpu.make_async_copy(src, own.at[lax.rem(i, slots), q], own_sem.at[lax.rem(i, slots), q])

    def core_copy(i, q):
        return pltpu.make_async_remote_copy(
            src_ref=p_ref.at[:, :, :, 1 - core, q * chunks + i], dst_ref=from_core.at[i, q],
            send_sem=core_send.at[i, q], recv_sem=core_recv.at[i, q], device_id=partner, device_id_type=MESH,
        )

    def indices(q):
        one, two, three = ORDERS[q]
        here = {a: bits[a] for a in range(3)}
        there = {a: 1 - bits[a] for a in range(3)}
        rest = tuple(a for a in range(3) if a != one)
        a_full = at({one: there[one]}, (0, 1, 2))
        b_full = at({one: here[one], two: there[two]}, (0, 1, 2))
        b_in_a = at({two: there[two]}, rest)
        c_full = at({one: here[one], two: here[two], three: there[three]}, (0, 1, 2))
        c_in_a = at({two: here[two], three: there[three]}, rest)
        mine = at(here, (0, 1, 2))
        mine_in_a = at({two: here[two], three: here[three]}, rest)
        return a_full, b_full, b_in_a, c_full, c_in_a, (there[three],), mine, mine_in_a, (here[three],)

    def step_copy(i, q, stage):
        a_full, _, b_in_a, _, _, c_in_b, *_ = indices(q)
        src, dst, send, recv = (
            (from_core.at[(i, q) + a_full], from_a.at[i, q], a_send, a_recv),
            (from_a.at[(i, q) + b_in_a], from_b.at[i, q], b_send, b_recv),
            (from_b.at[(i, q) + c_in_b], from_c.at[i, q], c_send, c_recv),
        )[stage]
        return pltpu.make_async_remote_copy(
            src_ref=src, dst_ref=dst, send_sem=send.at[i, q], recv_sem=recv.at[i, q],
            device_id=neighbour(me, bits, ORDERS[q][stage]), device_id_type=MESH,
        )

    def add(parts):
        total = parts[0].astype(F32)
        for part in parts[1:]:
            total = total + part.astype(F32)
        return total

    for i in range(chunks):
        for q in range(3):
            core_copy(i, q).start()
            if i == 0:
                own_copy(i, q).start()
    square[...] = jnp.zeros_like(square)

    @pl.loop(0, g1_ref.shape[0])
    def _(b):
        wide = g1_ref[b].astype(F32)
        square[...] += fold(wide * wide)

    @pl.loop(0, chunks + 3)
    def _(s):
        @pl.when(s < chunks)
        def _():
            for q in range(3):
                own_copy(s, q).wait()
                core_copy(s, q).wait_recv()
                a_full = indices(q)[0]
                o, k = (lax.rem(s, slots), q) + a_full, (s, q) + a_full
                from_core[k] = add([own[o], from_core[k]]).astype(BF16)
                step_copy(s, q, 0).start()

        @pl.when((s >= 1) & (s < chunks + 1))
        def _():
            i = s - 1
            for q in range(3):
                step_copy(i, q, 0).wait_recv()
                _, b_full, b_in_a, *_ = indices(q)
                o, k, ka = (lax.rem(i, slots), q) + b_full, (i, q) + b_full, (i, q) + b_in_a
                from_a[ka] = add([own[o], from_core[k], from_a[ka]]).astype(BF16)
                step_copy(i, q, 1).start()

        @pl.when((s >= 2) & (s < chunks + 2))
        def _():
            i = s - 2
            for q in range(3):
                step_copy(i, q, 1).wait_recv()
                _, _, _, c_full, c_in_a, c_in_b, *_ = indices(q)
                o, k, ka, kb = (lax.rem(i, slots), q) + c_full, (i, q) + c_full, (i, q) + c_in_a, (i, q) + c_in_b
                from_b[kb] = add([own[o], from_core[k], from_a[ka], from_b[kb]]).astype(BF16)
                step_copy(i, q, 2).start()

        @pl.when(s >= 3)
        def _():
            i = s - 3
            for q in range(3):
                step_copy(i, q, 2).wait_recv()
                *_, mine, mine_in_a, mine_in_b = indices(q)
                o, k, ka, kb = (lax.rem(i, slots), q) + mine, (i, q) + mine, (i, q) + mine_in_a, (i, q) + mine_in_b
                g = add([own[o], from_core[k], from_a[ka], from_b[kb], from_c[i, q]]).astype(BF16)
                g_ref[q * chunks + i] = g
                wide = g.astype(F32)
                square[...] += fold(wide * wide)

        @pl.when(s + 1 < chunks)
        def _():
            for q in range(3):
                own_copy(s + 1, q).start()

    squares[me] = square[...]

    def square_copy(i):
        return pltpu.make_async_remote_copy(
            src_ref=square, dst_ref=squares.at[me], send_sem=sq_send.at[i], recv_sem=sq_recv.at[me],
            device_id={"dp": lax.rem(me + i, n)}, device_id_type=MESH,
        )

    def square_arrival(i):
        other = lax.rem(me + i, n)
        return pltpu.make_async_remote_copy(
            src_ref=square, dst_ref=squares.at[other], send_sem=sq_send.at[i], recv_sem=sq_recv.at[other],
            device_id={"dp": other}, device_id_type=MESH,
        )

    @pl.loop(1, n)
    def _(i):
        square_copy(i).start()

    @pl.loop(0, chunks)
    def _(i):
        for q in range(3):
            core_copy(i, q).wait_send()
            for stage in range(3):
                step_copy(i, q, stage).wait_send()

    @pl.loop(1, n)
    def _(i):
        square_copy(i).wait_send()
        square_arrival(i).wait_recv()

    total = squares[0]
    for i in range(1, n):
        total = total + squares[i]
    total_ref[...] = total


def fold(wide):
    rows, columns = wide.shape
    rows8 = wide[:8]
    for r in range(8, rows, 8):
        rows8 = rows8 + wide[r : r + 8]
    total = rows8[:, :128]
    for c in range(128, columns, 128):
        total = total + rows8[:, c : c + 128]
    return total


def reduce_scatter(p, g1):
    n, blocks, rows, d = p.shape
    chunks = blocks // 3
    sem = pltpu.SemaphoreType.DMA
    cells = lambda *lead: pltpu.VMEM(lead + (rows, d), BF16)
    return pl.pallas_call(
        functools.partial(reduce_kernel, n, chunks),
        in_specs=[pl.BlockSpec(memory_space=pl.ANY), pl.BlockSpec(memory_space=pltpu.VMEM)],
        out_specs=[pl.BlockSpec(memory_space=pltpu.VMEM)] * 2,
        out_shape=[jax.ShapeDtypeStruct((blocks, rows, d), BF16), jax.ShapeDtypeStruct((8, 128), F32)],
        scratch_shapes=[
            cells(4, 3, 2, 2, 2), cells(chunks, 3, 2, 2, 2), cells(chunks, 3, 2, 2), cells(chunks, 3, 2), cells(chunks, 3),
            pltpu.VMEM((8, 128), F32), pltpu.VMEM((n, 8, 128), F32), sem((4, 3)),
        ] + [sem((chunks, 3))] * 8 + [sem((n,))] * 2,
        compiler_params=pltpu.CompilerParams(vmem_limit_bytes=62 * MIB, collective_id=0, has_side_effects=True),
        cost_estimate=pl.CostEstimate(flops=200_000_000_000, bytes_accessed=6 * p.size, transcendentals=0),
        name="reduce_scatter",
    )(p.reshape(2, 2, 2, 2, blocks, rows, d), g1)


def adamw(w, m, v, g):
    m = 0.9 * m + 0.1 * g
    v = 0.95 * v + 0.05 * g * g
    step = m * lax.rsqrt(v + 1e-8) + 0.1 * w
    return (w - 0.02 * step).astype(BF16), m, v


def terms(x, dy, wg, wu, wd, n):
    a0 = normed(x)
    gate, up, act = gate_up(a0, wg, wu)
    h1, a1 = down(act, wd, x)
    dgate, dup, p1 = last_layer(a1, dy, wg, wu, wd, n)
    dh = to_input(dgate, dup, wg, wu, h1, dy)
    p0 = first_layer(gate, up, a0, dh, wd, n)
    return p1, p0


def unpacked(g, blocks):
    wide = lambda t: t.transpose(1, 0, 2).reshape(64, -1)
    return wide(g[blocks : 2 * blocks]), wide(g[2 * blocks :]), g[:blocks].reshape(-1, g.shape[-1])


def solution(mesh):
    n = mesh.shape["dp"]

    def step(x, dy, *arrays):
        w, m, v = (arrays[i : i + 3] for i in (0, 3, 6))
        packed = terms(x[0], dy[0], *w, n)
        blocks = packed[0].shape[1] // 3
        g1 = lax.psum_scatter(packed[0], "dp", scatter_dimension=0, tiled=True)[0]
        g0, squares = reduce_scatter(packed[1], g1)
        by_layer = [[g.astype(F32) for g in unpacked(s, blocks)] for s in (g0, g1)]
        count = sum(a.size for a in w)
        square = jnp.sum(squares)
        factor = jnp.minimum(1.0, 0.5 * lax.rsqrt(square / count + 1e-30))
        me = lax.axis_index("dp")
        new = [[], [], []]
        for i in range(3):
            rows = m[i].shape[1]
            each = []
            for layer in range(2):
                own = lax.dynamic_slice(w[i], (layer, me * rows, 0), (1, rows, w[i].shape[2]))[0].astype(F32)
                each.append(adamw(own, m[i][layer], v[i][layer], by_layer[layer][i] * factor))
            gathered = [lax.all_gather(e[0], "dp", axis=0, tiled=True) for e in each]
            new[0].append(jnp.stack(gathered))
            new[1].append(jnp.stack([e[1] for e in each]))
            new[2].append(jnp.stack([e[2] for e in each]))
        return tuple(new[0] + new[1] + new[2])

    rows, all_ = P("dp"), P()
    moment, out_moment = P(None, "dp"), P("rep", "dp")
    return jax.shard_map(
        step,
        mesh=mesh,
        in_specs=(rows, rows) + (all_,) * 3 + (moment,) * 6,
        out_specs=(P("rep"),) * 3 + (out_moment,) * 6,
        check_vma=False,
    )
```

```python
import functools

import jax
import jax.numpy as jnp
from jax import lax
from jax.experimental import pallas as pl
from jax.experimental.pallas import tpu as pltpu
from jax.sharding import PartitionSpec as P

F32, BF16 = jnp.float32, jnp.bfloat16
EPS = 1e-6
MIB = 1 << 20


def dot(a, b, ca, cb):
    return lax.dot_general(a, b, (((ca,), (cb,)), ((), ())), preferred_element_type=F32)


def call(kernel, flops, nbytes, vmem, **kw):
    return pl.pallas_call(
        kernel,
        compiler_params=pltpu.CompilerParams(vmem_limit_bytes=vmem * MIB, dimension_semantics=("arbitrary",)),
        cost_estimate=pl.CostEstimate(flops=flops, bytes_accessed=nbytes, transcendentals=0),
        **kw,
    )


def whole(*shape):
    return pl.BlockSpec(shape, lambda i: (0,) * len(shape), pipeline_mode=pl.Buffered(1))


def normed(h):
    wide = h.astype(F32)
    return (wide * lax.rsqrt(jnp.mean(wide * wide, -1, keepdims=True) + EPS)).astype(BF16)


def first_forward_kernel(steps, parts, x_ref, wg_ref, wu_ref, wd_ref, gate_ref, up_ref, a_ref, h_ref, next_ref, total):
    k = pl.program_id(0)
    t = x_ref.shape[0]

    @pl.when(k == 0)
    def _():
        total[...] = jnp.zeros_like(total)

        @pl.loop(0, 8)
        def _(i):
            r = pl.ds(i * (t // 8), t // 8)
            a_ref[r, :] = normed(x_ref[r, :])

    for i in range(parts):
        r = pl.ds(i * (t // parts), t // parts)
        gate = dot(a_ref[r, :], wg_ref[0], 1, 0)
        up = dot(a_ref[r, :], wu_ref[0], 1, 0)
        gate_ref[r, :] = gate
        up_ref[r, :] = up
        total[r, :] += dot((gate * jax.nn.sigmoid(gate) * up).astype(BF16), wd_ref[0], 1, 0)

    @pl.when(k == steps - 1)
    def _():
        @pl.loop(0, 8)
        def _(i):
            r = pl.ds(i * (t // 8), t // 8)
            h = x_ref[r, :] + total[r, :].astype(BF16)
            h_ref[r, :] = h
            next_ref[r, :] = normed(h)


def first_forward(x, wg, wu, wd, bn=512, parts=2):
    t, d = x.shape
    f = wg.shape[2]
    steps = f // bn
    w = pl.BlockSpec((1, d, bn), lambda j: (0, 0, j))
    o = pl.BlockSpec((t, bn), lambda j: (0, j))
    return call(
        functools.partial(first_forward_kernel, steps, parts), 6 * t * d * f, 8 * t * f + 6 * d * f, 63,
        grid=(steps,),
        in_specs=[whole(t, d), w, w, pl.BlockSpec((1, bn, d), lambda j: (0, j, 0))],
        out_specs=[o, o] + [whole(t, d)] * 3,
        out_shape=[jax.ShapeDtypeStruct((t, f), F32)] * 2 + [jax.ShapeDtypeStruct((t, d), BF16)] * 3,
        scratch_shapes=[pltpu.VMEM((t, d), F32)],
        name="first_forward",
    )(x, wg, wu, wd)


def back_through_product(gate, up, dact):
    dact = dact.astype(BF16).astype(F32)
    sig = jax.nn.sigmoid(gate)
    silu = gate * sig
    dgate = dact * up * (sig + silu * (1.0 - sig))
    return (silu * up).astype(BF16), dgate.astype(BF16), (dact * silu).astype(BF16)


def put_terms(p_ref, stage_g, stage_u, stage_d, sems, j, steps, act, dgate, dup, a, dh, bn):
    n, blocks = p_ref.shape[:2]
    blocks = blocks // 3
    slot = lax.rem(j, 2)
    per = p_ref.shape[3] // bn

    def copies(slot, j):
        out = []
        for which, stage in enumerate((stage_g, stage_u)):
            part = p_ref.at[:, blocks * (1 + which) + lax.div(j, per), :, pl.ds(pl.multiple_of(lax.rem(j, per) * bn, bn), bn)]
            out.append(pltpu.make_async_copy(stage.at[slot], part, sems.at[slot, which]))
        first = j * (bn // 64)
        for i in range(bn // 64):
            to = p_ref.at[lax.div(first + i, blocks), lax.rem(first + i, blocks)]
            out.append(pltpu.make_async_copy(stage_d.at[slot, i], to, sems.at[slot, 2 + i]))
        return out

    @pl.when(j >= 2)
    def _():
        for c in copies(slot, j - 2):
            c.wait()

    for stage, cot in ((stage_g, dgate), (stage_u, dup)):
        stage[slot] = dot(a[...], cot, 0, 0).astype(BF16).reshape(stage.shape[1:])
    stage_d[slot] = dot(act, dh[...], 0, 0).astype(BF16).reshape(stage_d.shape[1:])
    for c in copies(slot, j):
        c.start()

    @pl.when(j == steps - 1)
    def _():
        for c in copies(1 - slot, j - 1) + copies(slot, j):
            c.wait()


def term_scratch(n, d, bn):
    return [
        pltpu.VMEM((2, n, d // n, bn), BF16),
        pltpu.VMEM((2, n, d // n, bn), BF16),
        pltpu.VMEM((2, bn // 64, 64, d), BF16),
        pltpu.SemaphoreType.DMA((2, 2 + bn // 64)),
    ]


def last_layer_kernel(steps, bn, parts, a_ref, dy_ref, wg_ref, wu_ref, wd_ref, dgate_ref, dup_ref, p_ref, act, *scratch):
    t = a_ref.shape[0]
    for i in range(parts):
        r = pl.ds(i * (t // parts), t // parts)
        gate = dot(a_ref[r, :], wg_ref[0], 1, 0)
        up = dot(a_ref[r, :], wu_ref[0], 1, 0)
        dact = dot(dy_ref[r, :], wd_ref[0], 1, 1)
        act[r, :], dgate_ref[r, :], dup_ref[r, :] = back_through_product(gate, up, dact)
    terms_of = act[...], dgate_ref[...], dup_ref[...]
    put_terms(p_ref, *scratch, pl.program_id(0), steps, *terms_of, a_ref, dy_ref, bn)


def last_layer(a, dy, wg, wu, wd, n, bn=512, parts=2):
    t, d = a.shape
    f = wg.shape[2]
    last = wg.shape[0] - 1
    steps = f // bn
    w = pl.BlockSpec((1, d, bn), lambda j: (last, 0, j))
    o = pl.BlockSpec((t, bn), lambda j: (0, j))
    return call(
        functools.partial(last_layer_kernel, steps, bn, parts), 12 * t * d * f, 4 * t * f + 12 * d * f, 63,
        grid=(steps,),
        in_specs=[whole(t, d), whole(t, d), w, w, pl.BlockSpec((1, bn, d), lambda j: (last, j, 0))],
        out_specs=[o, o, pl.BlockSpec(memory_space=pl.ANY)],
        out_shape=[jax.ShapeDtypeStruct((t, f), BF16)] * 2 + [jax.ShapeDtypeStruct((n, 3 * f // n // 64, 64, d), BF16)],
        scratch_shapes=[pltpu.VMEM((t, bn), BF16)] + term_scratch(n, d, bn),
        name="last_layer",
    )(a, dy, wg, wu, wd)


def to_input_kernel(dgate_ref, dup_ref, wg_ref, wu_ref, h_ref, dy_ref, dh_ref):
    da = dot(dgate_ref[...], wg_ref[0], 1, 1).astype(BF16) + dot(dup_ref[...], wu_ref[0], 1, 1).astype(BF16)
    da = da.astype(F32)
    wide = h_ref[...].astype(F32)
    scale = lax.rsqrt(jnp.mean(wide * wide, -1, keepdims=True) + EPS)
    inner = jnp.mean(da * wide, -1, keepdims=True)
    dwide = da * scale - wide * (scale * scale * scale * inner)
    dh_ref[...] = dy_ref[...] + dwide.astype(BF16)


def to_input(dgate, dup, wg, wu, h, dy, bm=256):
    t, f = dgate.shape
    d = h.shape[1]
    last = wg.shape[0] - 1
    c = pl.BlockSpec((bm, f), lambda i: (i, 0))
    r = pl.BlockSpec((bm, d), lambda i: (i, 0))
    w = pl.BlockSpec((1, d, f), lambda i: (last, 0, 0), pipeline_mode=pl.Buffered(1))
    return call(
        to_input_kernel, 4 * t * d * f, 4 * t * f + 4 * d * f, 60,
        grid=(t // bm,),
        in_specs=[c, c, w, w, r, r],
        out_specs=r,
        out_shape=jax.ShapeDtypeStruct((t, d), BF16),
        name="to_input",
    )(dgate, dup, wg, wu, h, dy)


def first_layer_kernel(steps, bn, gate_ref, up_ref, a_ref, dh_ref, wd_ref, p_ref, *scratch):
    dact = dot(dh_ref[...], wd_ref[0], 1, 1)
    act, dgate, dup = back_through_product(gate_ref[...], up_ref[...], dact)
    put_terms(p_ref, *scratch, pl.program_id(0), steps, act, dgate, dup, a_ref, dh_ref, bn)


def first_layer(gate, up, a, dh, wd, n, bn=512):
    t, d = a.shape
    f = gate.shape[1]
    steps = f // bn
    c = pl.BlockSpec((t, bn), lambda j: (0, j))
    return call(
        functools.partial(first_layer_kernel, steps, bn), 8 * t * d * f, 8 * t * f + 8 * d * f, 60,
        grid=(steps,),
        in_specs=[c, c, whole(t, d), whole(t, d), pl.BlockSpec((1, bn, d), lambda j: (0, j, 0))],
        out_specs=pl.BlockSpec(memory_space=pl.ANY),
        out_shape=jax.ShapeDtypeStruct((n, 3 * f // n // 64, 64, d), BF16),
        scratch_shapes=term_scratch(n, d, bn),
        name="first_layer",
    )(gate, up, a, dh, wd)


ORDERS = ((0, 1, 2), (1, 2, 0), (2, 0, 1))
MESH = pl.DeviceIdType.MESH


def place():
    me = lax.axis_index("dp")
    bits = (lax.rem(me // 8, 2), lax.rem(me // 4, 2), lax.rem(me // 2, 2))
    return me, bits, lax.rem(me, 2)


def neighbour(me, bits, axis):
    step = (8, 4, 2)[axis]
    return {"dp": me + step * (1 - 2 * bits[axis])}


def greet_all(me, n):
    barrier = pltpu.get_barrier_semaphore()

    @pl.loop(1, n)
    def _(i):
        pl.semaphore_signal(barrier, inc=1, device_id={"dp": lax.rem(me + i, n)}, device_id_type=MESH)

    pl.semaphore_wait(barrier, n - 1)


def at(fixed, among):
    return tuple(fixed.get(a, slice(None)) for a in among)


def reduce_kernel(
    n, chunks, p_ref, g1_ref, g_ref, total_ref, own, from_core, from_a, from_b, from_c, square, squares,
    own_sem, core_send, core_recv, a_send, a_recv, b_send, b_recv, c_send, c_recv, sq_send, sq_recv,
):
    me, bits, core = place()
    partner = {"dp": me + 1 - 2 * core}
    slots = own.shape[0]
    greet_all(me, n)

    def own_copy(i, q):
        src = p_ref.at[:, :, :, core, q * chunks + i]
        return pltpu.make_async_copy(src, own.at[lax.rem(i, slots), q], own_sem.at[lax.rem(i, slots), q])

    def core_copy(i, q):
        return pltpu.make_async_remote_copy(
            src_ref=p_ref.at[:, :, :, 1 - core, q * chunks + i], dst_ref=from_core.at[i, q],
            send_sem=core_send.at[i, q], recv_sem=core_recv.at[i, q], device_id=partner, device_id_type=MESH,
        )

    def indices(q):
        one, two, three = ORDERS[q]
        here = {a: bits[a] for a in range(3)}
        there = {a: 1 - bits[a] for a in range(3)}
        rest = tuple(a for a in range(3) if a != one)
        a_full = at({one: there[one]}, (0, 1, 2))
        b_full = at({one: here[one], two: there[two]}, (0, 1, 2))
        b_in_a = at({two: there[two]}, rest)
        c_full = at({one: here[one], two: here[two], three: there[three]}, (0, 1, 2))
        c_in_a = at({two: here[two], three: there[three]}, rest)
        mine = at(here, (0, 1, 2))
        mine_in_a = at({two: here[two], three: here[three]}, rest)
        return a_full, b_full, b_in_a, c_full, c_in_a, (there[three],), mine, mine_in_a, (here[three],)

    def step_copy(i, q, stage):
        a_full, _, b_in_a, _, _, c_in_b, *_ = indices(q)
        src, dst, send, recv = (
            (from_core.at[(i, q) + a_full], from_a.at[i, q], a_send, a_recv),
            (from_a.at[(i, q) + b_in_a], from_b.at[i, q], b_send, b_recv),
            (from_b.at[(i, q) + c_in_b], from_c.at[i, q], c_send, c_recv),
        )[stage]
        return pltpu.make_async_remote_copy(
            src_ref=src, dst_ref=dst, send_sem=send.at[i, q], recv_sem=recv.at[i, q],
            device_id=neighbour(me, bits, ORDERS[q][stage]), device_id_type=MESH,
        )

    def add(parts):
        total = parts[0].astype(F32)
        for part in parts[1:]:
            total = total + part.astype(F32)
        return total

    for i in range(chunks):
        for q in range(3):
            core_copy(i, q).start()
            if i == 0:
                own_copy(i, q).start()
    square[...] = jnp.zeros_like(square)

    @pl.loop(0, g1_ref.shape[0])
    def _(b):
        g_ref[1, b] = g1_ref[b]
        wide = g1_ref[b].astype(F32)
        square[...] += fold(wide * wide)

    @pl.loop(0, chunks + 3)
    def _(s):
        @pl.when(s < chunks)
        def _():
            for q in range(3):
                own_copy(s, q).wait()
                core_copy(s, q).wait_recv()
                a_full = indices(q)[0]
                o, k = (lax.rem(s, slots), q) + a_full, (s, q) + a_full
                from_core[k] = add([own[o], from_core[k]]).astype(BF16)
                step_copy(s, q, 0).start()

        @pl.when((s >= 1) & (s < chunks + 1))
        def _():
            i = s - 1
            for q in range(3):
                step_copy(i, q, 0).wait_recv()
                _, b_full, b_in_a, *_ = indices(q)
                o, k, ka = (lax.rem(i, slots), q) + b_full, (i, q) + b_full, (i, q) + b_in_a
                from_a[ka] = add([own[o], from_core[k], from_a[ka]]).astype(BF16)
                step_copy(i, q, 1).start()

        @pl.when((s >= 2) & (s < chunks + 2))
        def _():
            i = s - 2
            for q in range(3):
                step_copy(i, q, 1).wait_recv()
                _, _, _, c_full, c_in_a, c_in_b, *_ = indices(q)
                o, k, ka, kb = (lax.rem(i, slots), q) + c_full, (i, q) + c_full, (i, q) + c_in_a, (i, q) + c_in_b
                from_b[kb] = add([own[o], from_core[k], from_a[ka], from_b[kb]]).astype(BF16)
                step_copy(i, q, 2).start()

        @pl.when(s >= 3)
        def _():
            i = s - 3
            for q in range(3):
                step_copy(i, q, 2).wait_recv()
                *_, mine, mine_in_a, mine_in_b = indices(q)
                o, k, ka, kb = (lax.rem(i, slots), q) + mine, (i, q) + mine, (i, q) + mine_in_a, (i, q) + mine_in_b
                g = add([own[o], from_core[k], from_a[ka], from_b[kb], from_c[i, q]]).astype(BF16)
                g_ref[0, q * chunks + i] = g
                wide = g.astype(F32)
                square[...] += fold(wide * wide)

        @pl.when(s + 1 < chunks)
        def _():
            for q in range(3):
                own_copy(s + 1, q).start()

    squares[me] = square[...]

    def square_copy(i):
        return pltpu.make_async_remote_copy(
            src_ref=square, dst_ref=squares.at[me], send_sem=sq_send.at[i], recv_sem=sq_recv.at[me],
            device_id={"dp": lax.rem(me + i, n)}, device_id_type=MESH,
        )

    def square_arrival(i):
        other = lax.rem(me + i, n)
        return pltpu.make_async_remote_copy(
            src_ref=square, dst_ref=squares.at[other], send_sem=sq_send.at[i], recv_sem=sq_recv.at[other],
            device_id={"dp": other}, device_id_type=MESH,
        )

    @pl.loop(1, n)
    def _(i):
        square_copy(i).start()

    @pl.loop(0, chunks)
    def _(i):
        for q in range(3):
            core_copy(i, q).wait_send()
            for stage in range(3):
                step_copy(i, q, stage).wait_send()

    @pl.loop(1, n)
    def _(i):
        square_copy(i).wait_send()
        square_arrival(i).wait_recv()

    total = squares[0]
    for i in range(1, n):
        total = total + squares[i]
    total_ref[...] = total


def fold(wide):
    rows, columns = wide.shape
    rows8 = wide[:8]
    for r in range(8, rows, 8):
        rows8 = rows8 + wide[r : r + 8]
    total = rows8[:, :128]
    for c in range(128, columns, 128):
        total = total + rows8[:, c : c + 128]
    return total


def reduce_scatter(p, g1):
    n, blocks, rows, d = p.shape
    chunks = blocks // 3
    sem = pltpu.SemaphoreType.DMA
    cells = lambda *lead: pltpu.VMEM(lead + (rows, d), BF16)
    return pl.pallas_call(
        functools.partial(reduce_kernel, n, chunks),
        in_specs=[pl.BlockSpec(memory_space=pl.ANY), pl.BlockSpec(memory_space=pltpu.VMEM)],
        out_specs=[pl.BlockSpec(memory_space=pltpu.VMEM)] * 2,
        out_shape=[jax.ShapeDtypeStruct((2, blocks, rows, d), BF16), jax.ShapeDtypeStruct((8, 128), F32)],
        scratch_shapes=[
            cells(4, 3, 2, 2, 2), cells(chunks, 3, 2, 2, 2), cells(chunks, 3, 2, 2), cells(chunks, 3, 2), cells(chunks, 3),
            pltpu.VMEM((8, 128), F32), pltpu.VMEM((n, 8, 128), F32), sem((4, 3)),
        ] + [sem((chunks, 3))] * 8 + [sem((n,))] * 2,
        compiler_params=pltpu.CompilerParams(vmem_limit_bytes=62 * MIB, collective_id=0, has_side_effects=True),
        cost_estimate=pl.CostEstimate(flops=200_000_000_000, bytes_accessed=6 * p.size, transcendentals=0),
        name="reduce_scatter",
    )(p.reshape(2, 2, 2, 2, blocks, rows, d), g1)


def moments_of(m, v, g):
    return 0.9 * m + 0.1 * g, 0.95 * v + 0.05 * g * g


def factor_of(sq_ref, count):
    square = jnp.sum(sq_ref[...], keepdims=True)
    return jnp.minimum(1.0, 0.5 * lax.rsqrt(square / count + 1e-30))


def new_weights_kernel(count, me_ref, sq_ref, *refs):
    factor = factor_of(sq_ref, count)
    for i in range(3):
        m_ref, v_ref, g_ref, w_ref, out_ref = refs[i::3]
        m, v = moments_of(m_ref[0], v_ref[0], g_ref[0, 0].astype(F32) * factor)
        w = w_ref[0].astype(F32)
        out_ref[0] = (w - 0.02 * (m * lax.rsqrt(v + 1e-8) + 0.1 * w)).astype(BF16)


def new_moments_kernel(count, me_ref, sq_ref, *refs):
    factor = factor_of(sq_ref, count)
    for i in range(3):
        m_ref, v_ref, g_ref, new_m_ref, new_v_ref = refs[i::3]
        new_m_ref[0], new_v_ref[0] = moments_of(m_ref[0], v_ref[0], g_ref[0, 0].astype(F32) * factor)


def update(kernel, name, me, squares, m, v, g, count, w, dtypes):
    layers, blocks, rows, d = g.shape
    per = blocks // 3
    wide = lambda row: pl.BlockSpec((1, rows, d), lambda l, j, me: (l, row(me), j))
    tall = lambda first: pl.BlockSpec((1, rows, d), lambda l, j, me: (l, first(me) + j, 0))
    zero, own = (lambda me: 0), (lambda me: me[0])
    in_place = [wide(zero), wide(zero), tall(zero)]
    of_g = [pl.BlockSpec((1, 1, rows, d), lambda l, j, me, k=k: (l, k * per + j, 0, 0)) for k in (1, 2, 0)]
    of_w = [wide(own), wide(own), tall(lambda me: me[0] * per)] if w else []
    return pl.pallas_call(
        functools.partial(kernel, float(count)),
        grid_spec=pltpu.PrefetchScalarGridSpec(
            num_scalar_prefetch=1,
            grid=(layers, per),
            in_specs=[pl.BlockSpec((8, 128), lambda l, j, me: (0, 0))] + in_place * 2 + of_g + of_w,
            out_specs=in_place * len(dtypes),
        ),
        out_shape=[jax.ShapeDtypeStruct(a.shape, dtype) for dtype in dtypes for a in m],
        compiler_params=pltpu.CompilerParams(vmem_limit_bytes=60 * MIB, dimension_semantics=("arbitrary",) * 2),
        cost_estimate=pl.CostEstimate(flops=20_000_000_000, bytes_accessed=20 * sum(a.size for a in m), transcendentals=0),
        name=name,
    )(me, squares, *m, *v, g, g, g, *w)


def copy_kernel(a_ref, b_ref, a_out, b_out):
    a_out[...] = a_ref[...]
    b_out[...] = b_ref[...]


def copied(a, b, rows=256):
    layers, n, columns = a.shape
    block = pl.BlockSpec((1, rows, columns), lambda l, i: (l, i, 0))
    return pl.pallas_call(
        copy_kernel,
        grid=(layers, n // rows),
        in_specs=[block] * 2,
        out_specs=[block] * 2,
        out_shape=[jax.ShapeDtypeStruct(a.shape, a.dtype)] * 2,
        compiler_params=pltpu.CompilerParams(vmem_limit_bytes=60 * MIB, dimension_semantics=("arbitrary",) * 2),
        cost_estimate=pl.CostEstimate(flops=20_000_000_000, bytes_accessed=8 * a.size, transcendentals=0),
        name="copied",
    )(a, b)


def gather_kernel(n, layers, pieces, gate_ref, up_ref, full_gate, full_up, own_sem, *sems):
    me, bits, core = place()
    partner = {"dp": me + 1 - 2 * core}
    width = gate_ref.shape[2] // (3 * pieces)
    chunks = [(l, k, which) for l in range(layers) for k in range(pieces) for which in range(2)]
    mine = (gate_ref, up_ref)
    full = (full_gate, full_up)
    greet_all(me, n)

    def region(i, q, free):
        l, k, which = chunks[i]
        lead = tuple(slice(None) if a in free else bits[a] for a in range(3))
        return full[which].at[(l,) + lead + (core, slice(None), pl.ds((3 * k + q) * width, width))]

    def source(i, q):
        l, k, which = chunks[i]
        return mine[which].at[l, :, pl.ds((3 * k + q) * width, width)]

    def own_copy(i, q):
        return pltpu.make_async_copy(source(i, q), region(i, q, ()), own_sem.at[i, q])

    def copy(i, q, stage):
        order = ORDERS[q]
        part = region(i, q, order[:stage])
        return pltpu.make_async_remote_copy(
            src_ref=source(i, q) if stage == 0 else part, dst_ref=part,
            send_sem=sems[2 * stage].at[i, q], recv_sem=sems[2 * stage + 1].at[i, q],
            device_id=partner if stage == 3 else neighbour(me, bits, order[stage]), device_id_type=MESH,
        )

    for s in range(len(chunks) + 3):
        for stage in range(4):
            i = s - stage
            if 0 <= i < len(chunks):
                for q in range(3):
                    if stage == 0:
                        own_copy(i, q).start()
                    else:
                        copy(i, q, stage - 1).wait_recv()
                        if stage == 1:
                            own_copy(i, q).wait()
                    copy(i, q, stage).start()
    for i in range(len(chunks)):
        for q in range(3):
            for stage in range(4):
                copy(i, q, stage).wait_send()
            copy(i, q, 3).wait_recv()


def gather(gate, up, n, pieces=2):
    layers, rows, columns = gate.shape
    sem = pltpu.SemaphoreType.DMA
    chunks = layers * pieces * 2
    full = jax.ShapeDtypeStruct((layers, 2, 2, 2, 2, rows, columns), BF16)
    out = pl.pallas_call(
        functools.partial(gather_kernel, n, layers, pieces),
        in_specs=[pl.BlockSpec(memory_space=pltpu.VMEM)] * 2,
        out_specs=[pl.BlockSpec(memory_space=pl.ANY)] * 2,
        out_shape=[full] * 2,
        scratch_shapes=[sem((chunks, 3))] * 9,
        compiler_params=pltpu.CompilerParams(vmem_limit_bytes=60 * MIB, collective_id=1, has_side_effects=True),
        cost_estimate=pl.CostEstimate(flops=200_000_000_000, bytes_accessed=6 * n * gate.size, transcendentals=0),
        name="gather",
    )(gate, up)
    return [o.reshape(layers, n * rows, columns) for o in out]


def terms(x, dy, wg, wu, wd, n):
    gate, up, a0, h1, a1 = first_forward(x, wg, wu, wd)
    dgate, dup, p1 = last_layer(a1, dy, wg, wu, wd, n)
    dh = to_input(dgate, dup, wg, wu, h1, dy)
    p0 = first_layer(gate, up, a0, dh, wd, n)
    return p1, p0


def solution(mesh):
    n = mesh.shape["dp"]

    def step(x, dy, *arrays):
        w, m, v = (arrays[i : i + 3] for i in (0, 3, 6))
        p1, p0 = terms(x[0], dy[0], *w, n)
        g1 = lax.psum_scatter(p1, "dp", scatter_dimension=0, tiled=True)[0]
        g, squares = reduce_scatter(p0, g1)
        me = lax.axis_index("dp").astype(jnp.int32).reshape(1)
        count = sum(a.size for a in w)
        gate, up, down_ = update(new_weights_kernel, "new_weights", me, squares, m, v, g, count, w, [BF16])
        gate, up = gather(gate, up, n)
        gate, up, down_, g = lax.optimization_barrier((gate, up, down_, g))
        down_ = lax.all_gather(down_, "dp", axis=1, tiled=True)
        gate, up = copied(gate, up)
        moments = update(new_moments_kernel, "new_moments", me, squares, m, v, g, count, (), [F32] * 2)
        return gate, up, down_, *moments

    rows, all_ = P("dp"), P()
    moment, out_moment = P(None, "dp"), P("rep", "dp")
    return jax.shard_map(
        step,
        mesh=mesh,
        in_specs=(rows, rows) + (all_,) * 3 + (moment,) * 6,
        out_specs=(P("rep"),) * 3 + (out_moment,) * 6,
        check_vma=False,
    )
```

```python
import functools

import jax
import jax.numpy as jnp
from jax import lax
from jax.experimental import pallas as pl
from jax.experimental.pallas import tpu as pltpu
from jax.sharding import PartitionSpec as P

F32, BF16 = jnp.float32, jnp.bfloat16
EPS = 1e-6
MIB = 1 << 20


def dot(a, b, ca, cb):
    return lax.dot_general(a, b, (((ca,), (cb,)), ((), ())), preferred_element_type=F32)


def call(kernel, flops, nbytes, vmem, **kw):
    return pl.pallas_call(
        kernel,
        compiler_params=pltpu.CompilerParams(vmem_limit_bytes=vmem * MIB, dimension_semantics=("arbitrary",)),
        cost_estimate=pl.CostEstimate(flops=flops, bytes_accessed=nbytes, transcendentals=0),
        **kw,
    )


def whole(*shape):
    return pl.BlockSpec(shape, lambda i: (0,) * len(shape), pipeline_mode=pl.Buffered(1))


def normed(h):
    wide = h.astype(F32)
    return (wide * lax.rsqrt(jnp.mean(wide * wide, -1, keepdims=True) + EPS)).astype(BF16)


def first_forward_kernel(steps, parts, x_ref, wg_ref, wu_ref, wd_ref, gate_ref, up_ref, a_ref, h_ref, next_ref, total):
    k = pl.program_id(0)
    t = x_ref.shape[0]

    @pl.when(k == 0)
    def _():
        total[...] = jnp.zeros_like(total)

        @pl.loop(0, 8)
        def _(i):
            r = pl.ds(i * (t // 8), t // 8)
            a_ref[r, :] = normed(x_ref[r, :])

    for i in range(parts):
        r = pl.ds(i * (t // parts), t // parts)
        gate = dot(a_ref[r, :], wg_ref[0], 1, 0)
        up = dot(a_ref[r, :], wu_ref[0], 1, 0)
        gate_ref[r, :] = gate
        up_ref[r, :] = up
        total[r, :] += dot((gate * jax.nn.sigmoid(gate) * up).astype(BF16), wd_ref[0], 1, 0)

    @pl.when(k == steps - 1)
    def _():
        @pl.loop(0, 8)
        def _(i):
            r = pl.ds(i * (t // 8), t // 8)
            h = x_ref[r, :] + total[r, :].astype(BF16)
            h_ref[r, :] = h
            next_ref[r, :] = normed(h)


def first_forward(x, wg, wu, wd, bn=512, parts=2):
    t, d = x.shape
    f = wg.shape[2]
    steps = f // bn
    w = pl.BlockSpec((1, d, bn), lambda j: (0, 0, j))
    o = pl.BlockSpec((t, bn), lambda j: (0, j))
    return call(
        functools.partial(first_forward_kernel, steps, parts), 6 * t * d * f, 8 * t * f + 6 * d * f, 63,
        grid=(steps,),
        in_specs=[whole(t, d), w, w, pl.BlockSpec((1, bn, d), lambda j: (0, j, 0))],
        out_specs=[o, o] + [whole(t, d)] * 3,
        out_shape=[jax.ShapeDtypeStruct((t, f), F32)] * 2 + [jax.ShapeDtypeStruct((t, d), BF16)] * 3,
        scratch_shapes=[pltpu.VMEM((t, d), F32)],
        name="first_forward",
    )(x, wg, wu, wd)


def back_through_product(gate, up, dact):
    dact = dact.astype(BF16).astype(F32)
    sig = jax.nn.sigmoid(gate)
    silu = gate * sig
    dgate = dact * up * (sig + silu * (1.0 - sig))
    return (silu * up).astype(BF16), dgate.astype(BF16), (dact * silu).astype(BF16)


def put_terms(p_ref, stage_g, stage_u, stage_d, sems, j, steps, act, dgate, dup, a, dh, bn):
    n, blocks = p_ref.shape[:2]
    blocks = blocks // 3
    slot = lax.rem(j, 2)
    per = p_ref.shape[3] // bn

    def copies(slot, j):
        out = []
        for which, stage in enumerate((stage_g, stage_u)):
            part = p_ref.at[:, blocks * (1 + which) + lax.div(j, per), :, pl.ds(pl.multiple_of(lax.rem(j, per) * bn, bn), bn)]
            out.append(pltpu.make_async_copy(stage.at[slot], part, sems.at[slot, which]))
        first = j * (bn // 64)
        for i in range(bn // 64):
            to = p_ref.at[lax.div(first + i, blocks), lax.rem(first + i, blocks)]
            out.append(pltpu.make_async_copy(stage_d.at[slot, i], to, sems.at[slot, 2 + i]))
        return out

    @pl.when(j >= 2)
    def _():
        for c in copies(slot, j - 2):
            c.wait()

    for stage, cot in ((stage_g, dgate), (stage_u, dup)):
        stage[slot] = dot(a[...], cot, 0, 0).astype(BF16).reshape(stage.shape[1:])
    stage_d[slot] = dot(act, dh[...], 0, 0).astype(BF16).reshape(stage_d.shape[1:])
    for c in copies(slot, j):
        c.start()

    @pl.when(j == steps - 1)
    def _():
        for c in copies(1 - slot, j - 1) + copies(slot, j):
            c.wait()


def term_scratch(n, d, bn):
    return [
        pltpu.VMEM((2, n, d // n, bn), BF16),
        pltpu.VMEM((2, n, d // n, bn), BF16),
        pltpu.VMEM((2, bn // 64, 64, d), BF16),
        pltpu.SemaphoreType.DMA((2, 2 + bn // 64)),
    ]


def last_layer_kernel(steps, bn, parts, a_ref, dy_ref, wg_ref, wu_ref, wd_ref, dgate_ref, dup_ref, p_ref, act, *scratch):
    t = a_ref.shape[0]
    for i in range(parts):
        r = pl.ds(i * (t // parts), t // parts)
        gate = dot(a_ref[r, :], wg_ref[0], 1, 0)
        up = dot(a_ref[r, :], wu_ref[0], 1, 0)
        dact = dot(dy_ref[r, :], wd_ref[0], 1, 1)
        act[r, :], dgate_ref[r, :], dup_ref[r, :] = back_through_product(gate, up, dact)
    terms_of = act[...], dgate_ref[...], dup_ref[...]
    put_terms(p_ref, *scratch, pl.program_id(0), steps, *terms_of, a_ref, dy_ref, bn)


def last_layer(a, dy, wg, wu, wd, n, bn=512, parts=2):
    t, d = a.shape
    f = wg.shape[2]
    last = wg.shape[0] - 1
    steps = f // bn
    w = pl.BlockSpec((1, d, bn), lambda j: (last, 0, j))
    o = pl.BlockSpec((t, bn), lambda j: (0, j))
    return call(
        functools.partial(last_layer_kernel, steps, bn, parts), 12 * t * d * f, 4 * t * f + 12 * d * f, 63,
        grid=(steps,),
        in_specs=[whole(t, d), whole(t, d), w, w, pl.BlockSpec((1, bn, d), lambda j: (last, j, 0))],
        out_specs=[o, o, pl.BlockSpec(memory_space=pl.ANY)],
        out_shape=[jax.ShapeDtypeStruct((t, f), BF16)] * 2 + [jax.ShapeDtypeStruct((n, 3 * f // n // 64, 64, d), BF16)],
        scratch_shapes=[pltpu.VMEM((t, bn), BF16)] + term_scratch(n, d, bn),
        name="last_layer",
    )(a, dy, wg, wu, wd)


def to_input_kernel(dgate_ref, dup_ref, wg_ref, wu_ref, h_ref, dy_ref, dh_ref):
    da = dot(dgate_ref[...], wg_ref[0], 1, 1).astype(BF16) + dot(dup_ref[...], wu_ref[0], 1, 1).astype(BF16)
    da = da.astype(F32)
    wide = h_ref[...].astype(F32)
    scale = lax.rsqrt(jnp.mean(wide * wide, -1, keepdims=True) + EPS)
    inner = jnp.mean(da * wide, -1, keepdims=True)
    dwide = da * scale - wide * (scale * scale * scale * inner)
    dh_ref[...] = dy_ref[...] + dwide.astype(BF16)


def to_input(dgate, dup, wg, wu, h, dy, bm=256):
    t, f = dgate.shape
    d = h.shape[1]
    last = wg.shape[0] - 1
    c = pl.BlockSpec((bm, f), lambda i: (i, 0))
    r = pl.BlockSpec((bm, d), lambda i: (i, 0))
    w = pl.BlockSpec((1, d, f), lambda i: (last, 0, 0), pipeline_mode=pl.Buffered(1))
    return call(
        to_input_kernel, 4 * t * d * f, 4 * t * f + 4 * d * f, 60,
        grid=(t // bm,),
        in_specs=[c, c, w, w, r, r],
        out_specs=r,
        out_shape=jax.ShapeDtypeStruct((t, d), BF16),
        name="to_input",
    )(dgate, dup, wg, wu, h, dy)


def first_layer_kernel(steps, bn, gate_ref, up_ref, a_ref, dh_ref, wd_ref, p_ref, *scratch):
    dact = dot(dh_ref[...], wd_ref[0], 1, 1)
    act, dgate, dup = back_through_product(gate_ref[...], up_ref[...], dact)
    put_terms(p_ref, *scratch, pl.program_id(0), steps, act, dgate, dup, a_ref, dh_ref, bn)


def first_layer(gate, up, a, dh, wd, n, bn=512):
    t, d = a.shape
    f = gate.shape[1]
    steps = f // bn
    c = pl.BlockSpec((t, bn), lambda j: (0, j))
    return call(
        functools.partial(first_layer_kernel, steps, bn), 8 * t * d * f, 8 * t * f + 8 * d * f, 60,
        grid=(steps,),
        in_specs=[c, c, whole(t, d), whole(t, d), pl.BlockSpec((1, bn, d), lambda j: (0, j, 0))],
        out_specs=pl.BlockSpec(memory_space=pl.ANY),
        out_shape=jax.ShapeDtypeStruct((n, 3 * f // n // 64, 64, d), BF16),
        scratch_shapes=term_scratch(n, d, bn),
        name="first_layer",
    )(gate, up, a, dh, wd)


ORDERS = ((0, 1, 2), (1, 2, 0), (2, 0, 1))
MESH = pl.DeviceIdType.MESH


def place():
    me = lax.axis_index("dp")
    bits = (lax.rem(me // 8, 2), lax.rem(me // 4, 2), lax.rem(me // 2, 2))
    return me, bits, lax.rem(me, 2)


def neighbour(me, bits, axis):
    step = (8, 4, 2)[axis]
    return {"dp": me + step * (1 - 2 * bits[axis])}


def greet_all(me, n):
    barrier = pltpu.get_barrier_semaphore()

    @pl.loop(1, n)
    def _(i):
        pl.semaphore_signal(barrier, inc=1, device_id={"dp": lax.rem(me + i, n)}, device_id_type=MESH)

    pl.semaphore_wait(barrier, n - 1)


def at(fixed, among):
    return tuple(fixed.get(a, slice(None)) for a in among)


def reduce_kernel(
    n, chunks, p_ref, g1_ref, g_ref, total_ref, own, from_core, from_a, from_b, from_c, square, squares,
    own_sem, core_send, core_recv, a_send, a_recv, b_send, b_recv, c_send, c_recv, sq_send, sq_recv,
):
    me, bits, core = place()
    partner = {"dp": me + 1 - 2 * core}
    slots = own.shape[0]
    greet_all(me, n)

    def own_copy(i, q):
        src = p_ref.at[:, :, :, core, q * chunks + i]
        return pltpu.make_async_copy(src, own.at[lax.rem(i, slots), q], own_sem.at[lax.rem(i, slots), q])

    def core_copy(i, q):
        return pltpu.make_async_remote_copy(
            src_ref=p_ref.at[:, :, :, 1 - core, q * chunks + i], dst_ref=from_core.at[i, q],
            send_sem=core_send.at[i, q], recv_sem=core_recv.at[i, q], device_id=partner, device_id_type=MESH,
        )

    def indices(q):
        one, two, three = ORDERS[q]
        here = {a: bits[a] for a in range(3)}
        there = {a: 1 - bits[a] for a in range(3)}
        rest = tuple(a for a in range(3) if a != one)
        a_full = at({one: there[one]}, (0, 1, 2))
        b_full = at({one: here[one], two: there[two]}, (0, 1, 2))
        b_in_a = at({two: there[two]}, rest)
        c_full = at({one: here[one], two: here[two], three: there[three]}, (0, 1, 2))
        c_in_a = at({two: here[two], three: there[three]}, rest)
        mine = at(here, (0, 1, 2))
        mine_in_a = at({two: here[two], three: here[three]}, rest)
        return a_full, b_full, b_in_a, c_full, c_in_a, (there[three],), mine, mine_in_a, (here[three],)

    def step_copy(i, q, stage):
        a_full, _, b_in_a, _, _, c_in_b, *_ = indices(q)
        src, dst, send, recv = (
            (from_core.at[(i, q) + a_full], from_a.at[i, q], a_send, a_recv),
            (from_a.at[(i, q) + b_in_a], from_b.at[i, q], b_send, b_recv),
            (from_b.at[(i, q) + c_in_b], from_c.at[i, q], c_send, c_recv),
        )[stage]
        return pltpu.make_async_remote_copy(
            src_ref=src, dst_ref=dst, send_sem=send.at[i, q], recv_sem=recv.at[i, q],
            device_id=neighbour(me, bits, ORDERS[q][stage]), device_id_type=MESH,
        )

    def add(parts):
        total = parts[0].astype(F32)
        for part in parts[1:]:
            total = total + part.astype(F32)
        return total

    for i in range(chunks):
        for q in range(3):
            core_copy(i, q).start()
            if i == 0:
                own_copy(i, q).start()
    square[...] = jnp.zeros_like(square)

    @pl.loop(0, g1_ref.shape[0])
    def _(b):
        g_ref[1, b] = g1_ref[b]
        wide = g1_ref[b].astype(F32)
        square[...] += fold(wide * wide)

    @pl.loop(0, chunks + 3)
    def _(s):
        @pl.when(s < chunks)
        def _():
            for q in range(3):
                own_copy(s, q).wait()
                core_copy(s, q).wait_recv()
                a_full = indices(q)[0]
                o, k = (lax.rem(s, slots), q) + a_full, (s, q) + a_full
                from_core[k] = add([own[o], from_core[k]]).astype(BF16)
                step_copy(s, q, 0).start()

        @pl.when((s >= 1) & (s < chunks + 1))
        def _():
            i = s - 1
            for q in range(3):
                step_copy(i, q, 0).wait_recv()
                _, b_full, b_in_a, *_ = indices(q)
                o, k, ka = (lax.rem(i, slots), q) + b_full, (i, q) + b_full, (i, q) + b_in_a
                from_a[ka] = add([own[o], from_core[k], from_a[ka]]).astype(BF16)
                step_copy(i, q, 1).start()

        @pl.when((s >= 2) & (s < chunks + 2))
        def _():
            i = s - 2
            for q in range(3):
                step_copy(i, q, 1).wait_recv()
                _, _, _, c_full, c_in_a, c_in_b, *_ = indices(q)
                o, k, ka, kb = (lax.rem(i, slots), q) + c_full, (i, q) + c_full, (i, q) + c_in_a, (i, q) + c_in_b
                from_b[kb] = add([own[o], from_core[k], from_a[ka], from_b[kb]]).astype(BF16)
                step_copy(i, q, 2).start()

        @pl.when(s >= 3)
        def _():
            i = s - 3
            for q in range(3):
                step_copy(i, q, 2).wait_recv()
                *_, mine, mine_in_a, mine_in_b = indices(q)
                o, k, ka, kb = (lax.rem(i, slots), q) + mine, (i, q) + mine, (i, q) + mine_in_a, (i, q) + mine_in_b
                g = add([own[o], from_core[k], from_a[ka], from_b[kb], from_c[i, q]]).astype(BF16)
                g_ref[0, q * chunks + i] = g
                wide = g.astype(F32)
                square[...] += fold(wide * wide)

        @pl.when(s + 1 < chunks)
        def _():
            for q in range(3):
                own_copy(s + 1, q).start()

    squares[me] = square[...]

    def square_copy(i):
        return pltpu.make_async_remote_copy(
            src_ref=square, dst_ref=squares.at[me], send_sem=sq_send.at[i], recv_sem=sq_recv.at[me],
            device_id={"dp": lax.rem(me + i, n)}, device_id_type=MESH,
        )

    def square_arrival(i):
        other = lax.rem(me + i, n)
        return pltpu.make_async_remote_copy(
            src_ref=square, dst_ref=squares.at[other], send_sem=sq_send.at[i], recv_sem=sq_recv.at[other],
            device_id={"dp": other}, device_id_type=MESH,
        )

    @pl.loop(1, n)
    def _(i):
        square_copy(i).start()

    @pl.loop(0, chunks)
    def _(i):
        for q in range(3):
            core_copy(i, q).wait_send()
            for stage in range(3):
                step_copy(i, q, stage).wait_send()

    @pl.loop(1, n)
    def _(i):
        square_copy(i).wait_send()
        square_arrival(i).wait_recv()

    total = squares[0]
    for i in range(1, n):
        total = total + squares[i]
    total_ref[...] = total


def fold(wide):
    rows, columns = wide.shape
    rows8 = wide[:8]
    for r in range(8, rows, 8):
        rows8 = rows8 + wide[r : r + 8]
    total = rows8[:, :128]
    for c in range(128, columns, 128):
        total = total + rows8[:, c : c + 128]
    return total


def reduce_scatter(p, g1):
    n, blocks, rows, d = p.shape
    chunks = blocks // 3
    sem = pltpu.SemaphoreType.DMA
    cells = lambda *lead: pltpu.VMEM(lead + (rows, d), BF16)
    return pl.pallas_call(
        functools.partial(reduce_kernel, n, chunks),
        in_specs=[pl.BlockSpec(memory_space=pl.ANY), pl.BlockSpec(memory_space=pltpu.VMEM)],
        out_specs=[pl.BlockSpec(memory_space=pltpu.VMEM)] * 2,
        out_shape=[jax.ShapeDtypeStruct((2, blocks, rows, d), BF16), jax.ShapeDtypeStruct((8, 128), F32)],
        scratch_shapes=[
            cells(4, 3, 2, 2, 2), cells(chunks, 3, 2, 2, 2), cells(chunks, 3, 2, 2), cells(chunks, 3, 2), cells(chunks, 3),
            pltpu.VMEM((8, 128), F32), pltpu.VMEM((n, 8, 128), F32), sem((4, 3)),
        ] + [sem((chunks, 3))] * 8 + [sem((n,))] * 2,
        compiler_params=pltpu.CompilerParams(vmem_limit_bytes=62 * MIB, collective_id=0, has_side_effects=True),
        cost_estimate=pl.CostEstimate(flops=200_000_000_000, bytes_accessed=6 * p.size, transcendentals=0),
        name="reduce_scatter",
    )(p.reshape(2, 2, 2, 2, blocks, rows, d), g1)


def moments_of(m, v, g):
    return 0.9 * m + 0.1 * g, 0.95 * v + 0.05 * g * g


def factor_of(sq_ref, count):
    square = jnp.sum(sq_ref[...], keepdims=True)
    return jnp.minimum(1.0, 0.5 * lax.rsqrt(square / count + 1e-30))


def tiles(i, g_ref):
    _, count, rows, d = g_ref.shape
    for b in range(count):
        yield b, ((0, pl.ds(b * rows, rows), slice(None)) if i == 2 else (0, slice(None), pl.ds(b * d, d)))


def new_weights_kernel(count, me_ref, sq_ref, *refs):
    factor = factor_of(sq_ref, count)
    for i in range(3):
        m_ref, v_ref, g_ref, w_ref, out_ref = refs[i::3]
        for b, at_ in tiles(i, g_ref):
            m, v = moments_of(m_ref[at_], v_ref[at_], g_ref[0, b].astype(F32) * factor)
            w = w_ref[at_].astype(F32)
            out_ref[at_] = (w - 0.02 * (m * lax.rsqrt(v + 1e-8) + 0.1 * w)).astype(BF16)


def new_moments_kernel(count, me_ref, sq_ref, *refs):
    factor = factor_of(sq_ref, count)
    for i in range(3):
        m_ref, v_ref, g_ref, new_m_ref, new_v_ref = refs[i::3]
        for b, at_ in tiles(i, g_ref):
            new_m_ref[at_], new_v_ref[at_] = moments_of(m_ref[at_], v_ref[at_], g_ref[0, b].astype(F32) * factor)


def update(kernel, name, me, squares, m, v, g, count, w, dtypes, many=3):
    layers, blocks, rows, d = g.shape
    per = blocks // 3 // many
    wide = lambda row: pl.BlockSpec((1, rows, many * d), lambda l, j, me: (l, row(me), j))
    tall = lambda first: pl.BlockSpec((1, many * rows, d), lambda l, j, me: (l, first(me) + j, 0))
    zero, own = (lambda me: 0), (lambda me: me[0])
    in_place = [wide(zero), wide(zero), tall(zero)]
    of_g = [pl.BlockSpec((1, many, rows, d), lambda l, j, me, k=k: (l, k * per + j, 0, 0)) for k in (1, 2, 0)]
    of_w = [wide(own), wide(own), tall(lambda me: me[0] * per)] if w else []
    return pl.pallas_call(
        functools.partial(kernel, float(count)),
        grid_spec=pltpu.PrefetchScalarGridSpec(
            num_scalar_prefetch=1,
            grid=(layers, per),
            in_specs=[pl.BlockSpec((8, 128), lambda l, j, me: (0, 0))] + in_place * 2 + of_g + of_w,
            out_specs=in_place * len(dtypes),
        ),
        out_shape=[jax.ShapeDtypeStruct(a.shape, dtype) for dtype in dtypes for a in m],
        compiler_params=pltpu.CompilerParams(vmem_limit_bytes=60 * MIB, dimension_semantics=("arbitrary",) * 2),
        cost_estimate=pl.CostEstimate(flops=20_000_000_000, bytes_accessed=20 * sum(a.size for a in m), transcendentals=0),
        name=name,
    )(me, squares, *m, *v, g, g, g, *w)


def copy_kernel(a_ref, b_ref, c_ref, a_out, b_out, c_out):
    a_out[...] = a_ref[...]
    b_out[...] = b_ref[...]
    c_out[0] = c_ref[...]


def copied(a, b, c, steps=4):
    layers, n, columns = a.shape
    rows, tall = n // steps, c.shape[0] // (steps * layers)
    block = pl.BlockSpec((1, rows, columns), lambda l, i: (l, i, 0))
    return pl.pallas_call(
        copy_kernel,
        grid=(layers, steps),
        in_specs=[block] * 2 + [pl.BlockSpec((tall, c.shape[1]), lambda l, i: (l * steps + i, 0))],
        out_specs=[block] * 2 + [pl.BlockSpec((1, tall, c.shape[1]), lambda l, i: (0, l * steps + i, 0))],
        out_shape=[jax.ShapeDtypeStruct(a.shape, a.dtype)] * 2 + [jax.ShapeDtypeStruct((2,) + c.shape, c.dtype)],
        compiler_params=pltpu.CompilerParams(vmem_limit_bytes=60 * MIB, dimension_semantics=("arbitrary",) * 2),
        cost_estimate=pl.CostEstimate(flops=20_000_000_000, bytes_accessed=10 * a.size, transcendentals=0),
        name="copied",
    )(a, b, c)


def into_last_kernel(whole_ref, c_ref, out_ref):
    out_ref[0] = c_ref[...]


def into_last(both, c, rows=768):
    n, columns = c.shape
    return pl.pallas_call(
        into_last_kernel,
        grid=(n // rows,),
        in_specs=[pl.BlockSpec(memory_space=pl.ANY), pl.BlockSpec((rows, columns), lambda i: (i, 0))],
        out_specs=pl.BlockSpec((1, rows, columns), lambda i: (1, i, 0)),
        out_shape=jax.ShapeDtypeStruct(both.shape, both.dtype),
        input_output_aliases={0: 0},
        compiler_params=pltpu.CompilerParams(vmem_limit_bytes=40 * MIB, dimension_semantics=("arbitrary",)),
        cost_estimate=pl.CostEstimate(flops=5_000_000_000, bytes_accessed=4 * c.size, transcendentals=0),
        name="into_last",
    )(both, c)


def gather_kernel(n, layers, pieces, gate_ref, up_ref, down_ref, full_gate, full_up, full_down, own_sem, *sems):
    me, bits, core = place()
    partner = {"dp": me + 1 - 2 * core}
    width = gate_ref.shape[2] // (3 * pieces)
    height = down_ref.shape[1] // (3 * pieces)
    chunks = [(l, k, which) for l in range(layers) for k in range(pieces) for which in range(3) if which < 2 or l == 0]
    mine = (gate_ref, up_ref, down_ref)
    full = (full_gate, full_up, full_down)
    greet_all(me, n)

    def third(i, q):
        _, k, which = chunks[i]
        if which == 2:
            return pl.ds((3 * k + q) * height, height), slice(None)
        return slice(None), pl.ds((3 * k + q) * width, width)

    def region(i, q, free):
        l, _, which = chunks[i]
        lead = tuple(slice(None) if a in free else bits[a] for a in range(3))
        return full[which].at[(l,) + lead + (core,) + third(i, q)]

    def source(i, q):
        l, _, which = chunks[i]
        return mine[which].at[(l,) + third(i, q)]

    def own_copy(i, q):
        return pltpu.make_async_copy(source(i, q), region(i, q, ()), own_sem.at[i, q])

    def copy(i, q, stage):
        order = ORDERS[q]
        part = region(i, q, order[:stage])
        return pltpu.make_async_remote_copy(
            src_ref=source(i, q) if stage == 0 else part, dst_ref=part,
            send_sem=sems[2 * stage].at[i, q], recv_sem=sems[2 * stage + 1].at[i, q],
            device_id=partner if stage == 3 else neighbour(me, bits, order[stage]), device_id_type=MESH,
        )

    for s in range(len(chunks) + 3):
        for stage in range(4):
            i = s - stage
            if 0 <= i < len(chunks):
                for q in range(3):
                    if stage == 0:
                        own_copy(i, q).start()
                    else:
                        copy(i, q, stage - 1).wait_recv()
                        if stage == 1:
                            own_copy(i, q).wait()
                    copy(i, q, stage).start()
    for i in range(len(chunks)):
        for q in range(3):
            for stage in range(4):
                copy(i, q, stage).wait_send()
            copy(i, q, 3).wait_recv()


def gather(gate, up, down_, n, pieces=2):
    layers = gate.shape[0]
    sem = pltpu.SemaphoreType.DMA
    chunks = (layers * 2 + 1) * pieces
    full = lambda t, many: jax.ShapeDtypeStruct((many, 2, 2, 2, 2) + t.shape[1:], BF16)
    out = pl.pallas_call(
        functools.partial(gather_kernel, n, layers, pieces),
        in_specs=[pl.BlockSpec(memory_space=pltpu.VMEM)] * 3,
        out_specs=[pl.BlockSpec(memory_space=pl.ANY)] * 3,
        out_shape=[full(gate, layers), full(up, layers), full(down_, 1)],
        scratch_shapes=[sem((chunks, 3))] * 9,
        compiler_params=pltpu.CompilerParams(vmem_limit_bytes=60 * MIB, collective_id=1, has_side_effects=True),
        cost_estimate=pl.CostEstimate(flops=200_000_000_000, bytes_accessed=7 * n * gate.size, transcendentals=0),
        name="gather",
    )(gate, up, down_)
    return [o.reshape(o.shape[0], -1, o.shape[-1]) for o in out]


def terms(x, dy, wg, wu, wd, n):
    gate, up, a0, h1, a1 = first_forward(x, wg, wu, wd)
    dgate, dup, p1 = last_layer(a1, dy, wg, wu, wd, n)
    dh = to_input(dgate, dup, wg, wu, h1, dy)
    p0 = first_layer(gate, up, a0, dh, wd, n)
    return p1, p0


def solution(mesh):
    n = mesh.shape["dp"]

    def step(x, dy, *arrays):
        w, m, v = (arrays[i : i + 3] for i in (0, 3, 6))
        p1, p0 = terms(x[0], dy[0], *w, n)
        g1 = lax.psum_scatter(p1, "dp", scatter_dimension=0, tiled=True)[0]
        g, squares = reduce_scatter(p0, g1)
        me = lax.axis_index("dp").astype(jnp.int32).reshape(1)
        count = sum(a.size for a in w)
        gate, up, down_ = update(new_weights_kernel, "new_weights", me, squares, m, v, g, count, w, [BF16])
        gate, up, first = gather(gate, up, down_, n)
        gate, up, first, last, g = lax.optimization_barrier((gate, up, first, down_[1], g))
        last = lax.all_gather(last, "dp", axis=0, tiled=True)
        gate, up, down_ = copied(gate, up, first[0])
        moments = update(new_moments_kernel, "new_moments", me, squares, m, v, g, count, (), [F32] * 2)
        return gate, up, into_last(down_, last), *moments

    rows, all_ = P("dp"), P()
    moment, out_moment = P(None, "dp"), P("rep", "dp")
    return jax.shard_map(
        step,
        mesh=mesh,
        in_specs=(rows, rows) + (all_,) * 3 + (moment,) * 6,
        out_specs=(P("rep"),) * 3 + (out_moment,) * 6,
        check_vma=False,
    )
```
